32 devices in a mesh: band: 8 (over y, x, core), gblk: 4 (over z).
Axes of the slice: x: 2, y: 2, z: 4, core: 2. Of those that a mesh axis runs over, the one named last changes fastest.
Arguments:
- eps_inv: bfloat16 [2, 2, 8, 4, 512, 16384], P(None, None, None, 'gblk', None, 'band'), may hold values from -6 to 6
- pair_elements: bfloat16 [2, 1, 16, 16384], P(None, None, 'band'), may hold values from -0.046875 to 0.046875
Outputs:
- sigma_terms: float32 [2, 2, 1, 16], P(None, None, None, 'band')
The draws below stay inside these ranges and needn't reach their ends.
All inputs are finite; a program needn't handle non-finite values.
Results may differ from the reference program's by a relative error of at most 0.0003.
Values may be sent and summed in bfloat16 or wider, within the bound.
No kernel may reach another device: no remote copies, remote signals or barrier semaphores. Data moves between devices by JAX's collectives and lax.ppermute only.
A program may use at most 128 MiB of HBM per device.

```python
import jax
import jax.numpy as jnp

NG = 16384
TILE = 512
NFREQ = 2
NDIAG = 1
NBANDS = 16
ROUNDS = 8
N_GBLK = 4


def levels(own_key, dims, pieces, least, high):
    level = 1.0
    for dim, parts in pieces:
        heights = jax.random.uniform(jax.random.fold_in(jax.random.fold_in(own_key, 6), dim), (parts,), jnp.float32, least / len(pieces), high / len(pieces))
        level = level * jnp.repeat(jnp.exp(heights), dims[dim] // parts).reshape((-1,) + (1,) * (len(dims) - 1 - dim))
    return level


def centred(key, shape, deviation, bound, pieces=(), held_as=jnp.bfloat16):
    result = jax.random.normal(key, shape, jnp.float32) * deviation
    if len(pieces) > 0:
        result = levels(key, shape, pieces, -0.22, 0.18) * result
    return jnp.clip(result, min=-bound, max=bound).astype(held_as)


def setup_inputs(seed: int = 0) -> dict:
    arg_keys = jax.random.split(jax.random.key(seed), 3)
    return {
        "eps_inv": centred(arg_keys[0], (NFREQ, 2, ROUNDS, N_GBLK, TILE, NG), 1.0, 6.0, ((3, 4), (5, 8))),
        "pair_elements": centred(arg_keys[1], (2, NDIAG, NBANDS, NG), NG ** -0.5, 0.046875, ((2, 8),)),
    }


def reference(eps_inv, pair_elements):
    matrices = eps_inv.reshape(NFREQ, 2, NG, NG)
    flat = pair_elements.reshape(2 * NDIAG * NBANDS, NG)
    real_part = pair_elements[0].astype(jnp.float32)
    imag_part = pair_elements[1].astype(jnp.float32)
    results = []
    for frequency in range(NFREQ):
        along_a = jnp.dot(flat, matrices[frequency, 0].T, preferred_element_type=jnp.float32).reshape(2, NDIAG, NBANDS, NG)
        along_b = jnp.dot(flat, matrices[frequency, 1].T, preferred_element_type=jnp.float32).reshape(2, NDIAG, NBANDS, NG)
        image_re = along_a[0] - along_b[1]
        image_im = along_a[1] + along_b[0]
        sigma_re = jnp.sum(real_part * image_re + imag_part * image_im, axis=-1)
        sigma_im = jnp.sum(real_part * image_im - imag_part * image_re, axis=-1)
        results.append(jnp.stack([sigma_re, sigma_im]))
    return jnp.stack(results)
```

```python
import jax
import jax.numpy as jnp
from jax import lax
from jax.experimental import pallas as pl
from jax.experimental.pallas import tpu as pltpu
from jax.sharding import PartitionSpec as P

AXES = ("band", "gblk")


def pack_kernel(pair_ref, cols_ref, rows_ref, *, owners, width, tile_rows, rounds, groups):
    group = lax.axis_index("gblk")
    local = pair_ref.shape[2]
    for part in range(2):
        at = pl.ds(part * local, local)
        for owner in range(owners):
            cols_ref[owner, at, :] = pair_ref[part, 0, :, pl.ds(owner * width, width)]
        for r in range(rounds):
            start = pl.multiple_of((r * groups + group) * tile_rows, tile_rows)
            tile = pair_ref[part, 0, :, pl.ds(start, tile_rows)]
            for owner in range(owners):
                rows_ref[owner, at, pl.ds(r * tile_rows, tile_rows)] = tile


def image_kernel(cols_ref, a0_ref, b0_ref, a1_ref, b1_ref, out_ref, w_ref):
    owners, per, _ = cols_ref.shape
    half = per // 2
    own = owners * per

    @pl.when(pl.program_id(0) == 0)
    def _():
        zero = jnp.zeros((own, cols_ref.shape[2]), w_ref.dtype)
        for copy in range(2):
            for f in range(2):
                base = (2 * copy + f) * own
                w_ref[2 * (1 - f), pl.ds(base, own), :] = zero
                w_ref[2 * (1 - f) + 1, pl.ds(base, own), :] = zero
                for owner in range(owners):
                    re = cols_ref[owner, pl.ds(0, half), :]
                    im = cols_ref[owner, pl.ds(half, half), :]
                    at = base + owner * per
                    w_ref[2 * f, pl.ds(at, half), :] = re
                    w_ref[2 * f, pl.ds(at + half, half), :] = im
                    w_ref[2 * f + 1, pl.ds(at, half), :] = -im
                    w_ref[2 * f + 1, pl.ds(at + half, half), :] = re

    acc = None
    for j, x_ref in enumerate((a0_ref, b0_ref, a1_ref, b1_ref)):
        term = lax.dot_general(
            x_ref[0], w_ref[j], (((1,), (1,)), ((), ())), preferred_element_type=jnp.float32
        )
        acc = term if acc is None else acc + term
    high = acc.astype(jnp.bfloat16).astype(jnp.float32)
    lane = lax.broadcasted_iota(jnp.int32, acc.shape, 1)
    out_ref[...] = jnp.where(lane < acc.shape[1] // 2, high, acc - high).astype(jnp.bfloat16)


def sigma_kernel(rows_ref, image_ref, out_ref, flat_ref, *, groups):
    owners, per, _ = rows_ref.shape
    for owner in range(owners):
        flat_ref[pl.ds(owner * per, per), :] = rows_ref[owner]
    both = jnp.dot(flat_ref[...], image_ref[...], preferred_element_type=jnp.float32)
    for owner in range(owners):
        block = both[owner * per : (owner + 1) * per]
        for group in range(groups):
            out_ref[owner * groups + group] = block


def final_kernel(parts_ref, out_ref):
    _, per, lanes = parts_ref.shape
    half = per // 2
    owner = lax.axis_index("band")
    total = jnp.sum(parts_ref[...], axis=0)
    lane = lax.broadcasted_iota(jnp.int32, (1, lanes), 1)
    own = lanes // 4

    def pick(row, f, slot):
        at = f * own + owner * per + slot
        keep = jnp.logical_or(lane == at, lane == at + 2 * own)
        return jnp.sum(jnp.where(keep, total[row : row + 1], 0.0))

    for f in range(2):
        for l in range(half):
            out_ref[f, 0, 0, l] = pick(l, f, l) + pick(half + l, f, half + l)
            out_ref[f, 1, 0, l] = pick(l, f, half + l) - pick(half + l, f, l)


def shards(eps_inv, pair_elements):
    owners = lax.axis_size("band")
    groups = lax.axis_size("gblk")
    freqs, _, rounds, _, tile_rows, width = eps_inv.shape
    local = pair_elements.shape[2]
    rows = rounds * tile_rows
    per = 2 * local
    lanes = 2 * freqs * owners * per
    vmem = pl.BlockSpec(memory_space=pltpu.VMEM)

    def packing(*refs):
        pack_kernel(*refs, owners=owners, width=width, tile_rows=tile_rows, rounds=rounds, groups=groups)

    cols, picked = pl.pallas_call(
        packing,
        out_shape=(
            jax.ShapeDtypeStruct((owners, per, width), jnp.bfloat16),
            jax.ShapeDtypeStruct((owners, per, rows), jnp.bfloat16),
        ),
        in_specs=[vmem],
        out_specs=(vmem, vmem),
        name="pack",
    )(pair_elements)
    cols = lax.all_to_all(cols, "band", 0, 0, tiled=True)
    picked = lax.all_to_all(picked, "band", 0, 0, tiled=True)

    blocks = eps_inv.reshape(freqs * 2, rows, width)
    bm = min(256, rows)

    def block_of(j):
        return pl.BlockSpec((1, bm, width), lambda i, j=j: (j, i, 0))

    image = pl.pallas_call(
        image_kernel,
        grid=(rows // bm,),
        out_shape=jax.ShapeDtypeStruct((rows, lanes), jnp.bfloat16),
        in_specs=[pl.BlockSpec(cols.shape, lambda i: (0, 0, 0))] + [block_of(j) for j in range(4)],
        out_specs=pl.BlockSpec((bm, lanes), lambda i: (i, 0)),
        scratch_shapes=[pltpu.VMEM((4, lanes, width), jnp.bfloat16)],
        compiler_params=pltpu.CompilerParams(
            dimension_semantics=("arbitrary",), vmem_limit_bytes=40 * 2**20
        ),
        name="image",
    )(cols, blocks, blocks, blocks, blocks)

    def contracting(*refs):
        sigma_kernel(*refs, groups=groups)

    partial = pl.pallas_call(
        contracting,
        out_shape=jax.ShapeDtypeStruct((owners * groups, per, lanes), jnp.float32),
        in_specs=[vmem, vmem],
        out_specs=vmem,
        scratch_shapes=[pltpu.VMEM((owners * per, rows), jnp.bfloat16)],
        name="contract",
    )(picked, image)
    parts = lax.all_to_all(partial, AXES, 0, 0, tiled=True)
    return pl.pallas_call(
        final_kernel,
        out_shape=jax.ShapeDtypeStruct((freqs, 2, 1, local), jnp.float32),
        in_specs=[vmem],
        out_specs=pl.BlockSpec(memory_space=pltpu.SMEM),
        name="final",
    )(parts)


def solution(mesh):
    placed = (P(None, None, None, "gblk", None, "band"), P(None, None, "band", None))
    return jax.shard_map(
        shards, mesh=mesh, in_specs=placed, out_specs=P(None, None, None, "band"), check_vma=False
    )
```

```python
import jax
import jax.numpy as jnp
from jax import lax
from jax.experimental import pallas as pl
from jax.experimental.pallas import tpu as pltpu
from jax.sharding import PartitionSpec as P

AXES = ("band", "gblk")
BM = 1024


def pack_kernel(pair_ref, out_ref, *, owners, width, tile_rows, rounds, groups):
    group = lax.axis_index("gblk")
    local = pair_ref.shape[2]
    for part in range(2):
        at = pl.ds(part * local, local)
        for owner in range(owners):
            out_ref[owner, at, pl.ds(0, width)] = pair_ref[part, 0, :, pl.ds(owner * width, width)]
        for r in range(rounds):
            start = pl.multiple_of((r * groups + group) * tile_rows, tile_rows)
            tile = pair_ref[part, 0, :, pl.ds(start, tile_rows)]
            for owner in range(owners):
                out_ref[owner, at, pl.ds(width + r * tile_rows, tile_rows)] = tile


def image_kernel(pair_ref, a_ref, b_ref, out_ref, w_ref, flat_ref, sum_ref, *, width, groups):
    owners, per, _ = pair_ref.shape
    half = per // 2
    own = owners * per
    step = pl.program_id(0)
    steps = pl.num_programs(0)
    freqs = w_ref.shape[0] // 2
    bm = a_ref.shape[1]
    rows = flat_ref.shape[1]
    now = step // (rows // bm)

    @pl.when(step == 0)
    def _():
        sum_ref[...] = jnp.zeros_like(sum_ref)
        zero = jnp.zeros((own, width), w_ref.dtype)
        for copy in range(2):
            for f in range(freqs):
                base = (copy * freqs + f) * own
                for other in range(freqs):
                    if other != f:
                        w_ref[2 * other, pl.ds(base, own), :] = zero
                        w_ref[2 * other + 1, pl.ds(base, own), :] = zero
                for owner in range(owners):
                    re = pair_ref[owner, pl.ds(0, half), pl.ds(0, width)]
                    im = pair_ref[owner, pl.ds(half, half), pl.ds(0, width)]
                    at = base + owner * per
                    w_ref[2 * f, pl.ds(at, half), :] = re
                    w_ref[2 * f, pl.ds(at + half, half), :] = im
                    w_ref[2 * f + 1, pl.ds(at, half), :] = -im
                    w_ref[2 * f + 1, pl.ds(at + half, half), :] = re
        for owner in range(owners):
            flat_ref[pl.ds(owner * per, per), :] = pair_ref[owner, :, pl.ds(width, rows)]

    acc = None
    for part, block_ref in enumerate((a_ref, b_ref)):
        term = lax.dot_general(
            block_ref[0], w_ref[2 * now + part], (((1,), (1,)), ((), ())),
            preferred_element_type=jnp.float32,
        )
        acc = term if acc is None else acc + term
    high = acc.astype(jnp.bfloat16).astype(jnp.float32)
    lane = lax.broadcasted_iota(jnp.int32, acc.shape, 1)
    image = jnp.where(lane < acc.shape[1] // 2, high, acc - high).astype(jnp.bfloat16)
    at = pl.multiple_of((step % (rows // bm)) * bm, bm)
    sum_ref[...] += jnp.dot(flat_ref[:, pl.ds(at, bm)], image, preferred_element_type=jnp.float32)

    @pl.when(step == steps - 1)
    def _():
        for owner in range(owners):
            block = sum_ref[pl.ds(owner * per, per), :]
            for group in range(groups):
                out_ref[owner * groups + group] = block


def final_kernel(parts_ref, out_ref):
    _, per, lanes = parts_ref.shape
    half = per // 2
    owner = lax.axis_index("band")
    total = jnp.sum(parts_ref[...], axis=0)
    lane = lax.broadcasted_iota(jnp.int32, (1, lanes), 1)
    freqs = out_ref.shape[0]
    own = lanes // (2 * freqs)

    def pick(row, f, slot):
        at = f * own + owner * per + slot
        keep = jnp.logical_or(lane == at, lane == at + freqs * own)
        return jnp.sum(jnp.where(keep, total[row : row + 1], 0.0))

    for f in range(freqs):
        for l in range(half):
            out_ref[f, 0, 0, l] = pick(l, f, l) + pick(half + l, f, half + l)
            out_ref[f, 1, 0, l] = pick(l, f, half + l) - pick(half + l, f, l)


def shards(eps_inv, pair_elements):
    owners = lax.axis_size("band")
    groups = lax.axis_size("gblk")
    freqs, _, rounds, _, tile_rows, width = eps_inv.shape
    local = pair_elements.shape[2]
    rows = rounds * tile_rows
    per = 2 * local
    lanes = 2 * freqs * owners * per
    vmem = pl.BlockSpec(memory_space=pltpu.VMEM)

    def packing(*refs):
        pack_kernel(*refs, owners=owners, width=width, tile_rows=tile_rows, rounds=rounds, groups=groups)

    packed = pl.pallas_call(
        packing,
        out_shape=jax.ShapeDtypeStruct((owners, per, width + rows), jnp.bfloat16),
        in_specs=[vmem],
        out_specs=vmem,
        name="pack",
    )(pair_elements)
    spread = lax.all_to_all(packed, "band", 0, 0, tiled=True)

    blocks = eps_inv.reshape(freqs * 2, rows, width)
    bm = min(BM, rows)
    steps = rows // bm

    def block_of(part):
        return pl.BlockSpec((1, bm, width), lambda i: (2 * (i // steps) + part, i % steps, 0))

    def imaging(*refs):
        image_kernel(*refs, width=width, groups=groups)

    partial = pl.pallas_call(
        imaging,
        grid=(freqs * steps,),
        out_shape=jax.ShapeDtypeStruct((owners * groups, per, lanes), jnp.float32),
        in_specs=[vmem] + [block_of(0), block_of(1)],
        out_specs=vmem,
        scratch_shapes=[
            pltpu.VMEM((2 * freqs, lanes, width), jnp.bfloat16),
            pltpu.VMEM((owners * per, rows), jnp.bfloat16),
            pltpu.VMEM((owners * per, lanes), jnp.float32),
        ],
        compiler_params=pltpu.CompilerParams(
            dimension_semantics=("arbitrary",), vmem_limit_bytes=40 * 2**20
        ),
        name="image",
    )(spread, blocks, blocks)
    parts = lax.all_to_all(partial, AXES, 0, 0, tiled=True)
    return pl.pallas_call(
        final_kernel,
        out_shape=jax.ShapeDtypeStruct((freqs, 2, 1, local), jnp.float32),
        in_specs=[vmem],
        out_specs=pl.BlockSpec(memory_space=pltpu.SMEM),
        name="final",
    )(parts)


def solution(mesh):
    placed = (P(None, None, None, "gblk", None, "band"), P(None, None, "band", None))
    return jax.shard_map(
        shards, mesh=mesh, in_specs=placed, out_specs=P(None, None, None, "band"), check_vma=False
    )
```
